16 devices in a mesh: ep: 16 (over z, y, x, core).
Axes of the slice: x: 2, y: 2, z: 2, core: 2. Of those that a mesh axis runs over, the one named last changes fastest.
Arguments:
- hidden: bfloat16 [32768, 1280], P('ep')
- grad_out: bfloat16 [32768, 1280], P('ep')
- routes: int32 [32768, 6], P('ep')
- w_router: bfloat16 [1280, 64], replicated
- w_one: bfloat16 [64, 1280, 896], P('ep')
- w_three: bfloat16 [64, 1280, 896], P('ep')
- w_two: bfloat16 [64, 896, 1280], P('ep')
- shared_one: bfloat16 [1280, 1792], replicated
- shared_three: bfloat16 [1280, 1792], replicated
- shared_two: bfloat16 [1792, 1280], replicated
Outputs:
- output 1: bfloat16 [32768, 1280], P('ep')
- output 2: bfloat16 [32768, 1280], P('ep')
- output 3: float32 [1280, 64], replicated
- output 4: bfloat16 [64, 1280, 896], P('ep')
- output 5: bfloat16 [64, 1280, 896], P('ep')
- output 6: bfloat16 [64, 896, 1280], P('ep')
- output 7: float32 [1280, 1792], replicated
- output 8: float32 [1280, 1792], replicated
- output 9: float32 [1792, 1280], replicated
All inputs are finite; a program needn't handle non-finite values.
Results may differ from the reference program's by a relative error of at most 0.00199.
Values are sent between devices in bfloat16 or wider.
A program may use at most 1 GiB of HBM per device.

```python
import jax
import jax.numpy as jnp
from jax import lax

GROUP_SIZE = 16
TOKENS_DEV = 2048
D_MODEL = 1280
NUM_EXPERTS = 64
TOP_K = 6
EXPERT_FF = 896
SHARED_FF = 1792
HOT_COUNT = 4

ROUTE_SCALE = 2.5
TOKENS_ALL = GROUP_SIZE * TOKENS_DEV
CAPACITY = (5 * TOKENS_DEV * TOP_K + 4 * NUM_EXPERTS - 1) // (4 * NUM_EXPERTS)
HOT_BIAS = 2 ** 18
SCORE_RANGE = 2 ** 20


def draw_routes(route_key):
    key_hot, key_score = jax.random.split(route_key)
    hot_order = jax.random.permutation(key_hot, NUM_EXPERTS)
    hot_bias = jnp.zeros((NUM_EXPERTS,), jnp.int32).at[hot_order[:HOT_COUNT]].set(HOT_BIAS)
    scores = jax.random.randint(key_score, (TOKENS_ALL, NUM_EXPERTS), 0, SCORE_RANGE, jnp.int32) + hot_bias
    distinct = scores * NUM_EXPERTS + jnp.arange(NUM_EXPERTS, dtype=jnp.int32)
    top_vals, routes = lax.top_k(distinct, TOP_K)
    return routes.astype(jnp.int32)


def normal_weights(weight_key, shape, fan_in):
    return (jax.random.normal(weight_key, shape, jnp.float32) * fan_in ** -0.5).astype(jnp.bfloat16)


def setup_inputs(seed: int = 0) -> dict:
    key_list = jax.random.split(jax.random.key(seed), 11)
    hidden = jax.random.normal(key_list[0], (TOKENS_ALL, D_MODEL), jnp.float32)
    row_scale = 0.5 + jax.random.uniform(key_list[1], (TOKENS_ALL, 1), jnp.float32)
    grad_out = jax.random.normal(key_list[2], (TOKENS_ALL, D_MODEL), jnp.float32) * row_scale
    return {
        'hidden': hidden.astype(jnp.bfloat16),
        'grad_out': grad_out.astype(jnp.bfloat16),
        'routes': draw_routes(key_list[3]),
        'w_router': normal_weights(key_list[4], (D_MODEL, NUM_EXPERTS), D_MODEL),
        'w_one': normal_weights(key_list[5], (NUM_EXPERTS, D_MODEL, EXPERT_FF), D_MODEL),
        'w_three': normal_weights(key_list[6], (NUM_EXPERTS, D_MODEL, EXPERT_FF), D_MODEL),
        'w_two': normal_weights(key_list[7], (NUM_EXPERTS, EXPERT_FF, D_MODEL), EXPERT_FF),
        'shared_one': normal_weights(key_list[8], (D_MODEL, SHARED_FF), D_MODEL),
        'shared_three': normal_weights(key_list[9], (D_MODEL, SHARED_FF), D_MODEL),
        'shared_two': normal_weights(key_list[10], (SHARED_FF, D_MODEL), SHARED_FF),
    }


def silu_parts(pre_act):
    sig_val = jax.nn.sigmoid(pre_act)
    return pre_act * sig_val, sig_val * (1.0 + pre_act * (1.0 - sig_val))


def as_bf16(values):
    return values.astype(jnp.bfloat16).astype(jnp.float32)


def reference(hidden, grad_out, routes, w_router, w_one, w_three, w_two, shared_one, shared_three, shared_two):
    hidden_f = hidden.astype(jnp.float32)
    grad_f = grad_out.astype(jnp.float32)
    scores = jax.nn.sigmoid(jnp.dot(hidden, w_router, preferred_element_type=jnp.float32))
    picked = jnp.take_along_axis(scores, routes, axis=1)
    pick_sum = jnp.sum(picked, axis=1, keepdims=True)
    weights = ROUTE_SCALE * picked / pick_sum

    src_routes = routes.reshape(GROUP_SIZE, TOKENS_DEV, TOP_K)
    expert_ids = jnp.arange(NUM_EXPERTS, dtype=jnp.int32)
    hit_count = jnp.sum((src_routes[:, :, :, None] == expert_ids).astype(jnp.int32), axis=2)
    before = jnp.cumsum(hit_count, axis=1) - hit_count
    position = jnp.take_along_axis(before, src_routes, axis=2)
    slot_ids = jnp.where(position < CAPACITY, src_routes * CAPACITY + position, NUM_EXPERTS * CAPACITY)
    source_ids = jnp.broadcast_to(jnp.arange(GROUP_SIZE, dtype=jnp.int32)[:, None, None], slot_ids.shape)
    token_ids = jnp.broadcast_to(jnp.arange(TOKENS_DEV, dtype=jnp.int32)[None, :, None], slot_ids.shape)
    slot_token = jnp.full((GROUP_SIZE, NUM_EXPERTS * CAPACITY), TOKENS_DEV, jnp.int32).at[source_ids, slot_ids].set(token_ids, mode='drop')
    slot_weight = jnp.zeros((GROUP_SIZE, NUM_EXPERTS * CAPACITY), jnp.float32).at[source_ids, slot_ids].set(weights.reshape(GROUP_SIZE, TOKENS_DEV, TOP_K), mode='drop')
    slot_token_e = slot_token.reshape(GROUP_SIZE, NUM_EXPERTS, CAPACITY).transpose(1, 0, 2)
    slot_weight_e = slot_weight.reshape(GROUP_SIZE, NUM_EXPERTS, CAPACITY).transpose(1, 0, 2)

    zero_row = jnp.zeros((GROUP_SIZE, 1, D_MODEL), jnp.float32)
    hidden_pad = jnp.concatenate([hidden_f.reshape(GROUP_SIZE, TOKENS_DEV, D_MODEL), zero_row], axis=1)
    grad_pad = jnp.concatenate([grad_f.reshape(GROUP_SIZE, TOKENS_DEV, D_MODEL), zero_row], axis=1)
    gather_rows = jax.vmap(lambda row_table, row_ids: row_table[row_ids])
    src_rows = jnp.arange(GROUP_SIZE)[:, None]

    def expert_step(scan_carry, per_expert):
        out_acc, dx_acc, dot_acc = scan_carry
        slot_tok, slot_wt, one_mat, three_mat, two_mat, expert_id = per_expert
        one_full = one_mat.astype(jnp.float32)
        three_full = three_mat.astype(jnp.float32)
        two_full = two_mat.astype(jnp.float32)
        in_rows = gather_rows(hidden_pad, slot_tok)
        grad_rows = gather_rows(grad_pad, slot_tok)
        pre_one = jnp.einsum('gcd,df->gcf', in_rows, one_full)
        pre_three = jnp.einsum('gcd,df->gcf', in_rows, three_full)
        act_one, dact_one = silu_parts(pre_one)
        mid_act = as_bf16(act_one * pre_three)
        expert_out = as_bf16(jnp.einsum('gcf,fd->gcd', mid_act, two_full))
        grad_slot = as_bf16(slot_wt[:, :, None] * grad_rows)
        grad_mid = jnp.einsum('gcd,fd->gcf', grad_slot, two_full)
        grad_one = as_bf16(grad_mid * pre_three * dact_one)
        grad_three = as_bf16(grad_mid * act_one)
        wgrad_one = jnp.einsum('gcd,gcf->df', in_rows, grad_one).astype(jnp.bfloat16)
        wgrad_three = jnp.einsum('gcd,gcf->df', in_rows, grad_three).astype(jnp.bfloat16)
        wgrad_two = jnp.einsum('gcf,gcd->fd', mid_act, grad_slot).astype(jnp.bfloat16)
        dx_slot = as_bf16(jnp.einsum('gcf,df->gcd', grad_one, one_full) + jnp.einsum('gcf,df->gcd', grad_three, three_full))
        slot_dot = jnp.sum(grad_rows * expert_out, axis=2)
        out_acc = out_acc.at[src_rows, slot_tok].add(slot_wt[:, :, None] * expert_out, mode='drop')
        dx_acc = dx_acc.at[src_rows, slot_tok].add(dx_slot, mode='drop')
        dot_acc = dot_acc.at[src_rows, slot_tok, expert_id].add(slot_dot, mode='drop')
        return (out_acc, dx_acc, dot_acc), (wgrad_one, wgrad_three, wgrad_two)

    acc_init = (jnp.zeros((GROUP_SIZE, TOKENS_DEV, D_MODEL), jnp.float32), jnp.zeros((GROUP_SIZE, TOKENS_DEV, D_MODEL), jnp.float32), jnp.zeros((GROUP_SIZE, TOKENS_DEV, NUM_EXPERTS), jnp.float32))
    scan_out, expert_grads = lax.scan(expert_step, acc_init, (slot_token_e, slot_weight_e, w_one, w_three, w_two, expert_ids))
    out_acc, dx_acc, dot_acc = scan_out
    grad_w_one, grad_w_three, grad_w_two = expert_grads

    shared_pre_one = jnp.dot(hidden, shared_one, preferred_element_type=jnp.float32)
    shared_pre_three = jnp.dot(hidden, shared_three, preferred_element_type=jnp.float32)
    shared_act, shared_dact = silu_parts(shared_pre_one)
    shared_mid = (shared_act * shared_pre_three).astype(jnp.bfloat16)
    shared_out = jnp.dot(shared_mid, shared_two, preferred_element_type=jnp.float32)
    hidden_out = (hidden_f + shared_out + out_acc.reshape(TOKENS_ALL, D_MODEL)).astype(jnp.bfloat16)

    shared_grad_mid = jnp.dot(grad_out, shared_two.T, preferred_element_type=jnp.float32)
    shared_grad_one = (shared_grad_mid * shared_pre_three * shared_dact).astype(jnp.bfloat16)
    shared_grad_three = (shared_grad_mid * shared_act).astype(jnp.bfloat16)
    grad_shared_two = jnp.dot(shared_mid.T, grad_out, preferred_element_type=jnp.float32)
    grad_shared_one = jnp.dot(hidden.T, shared_grad_one, preferred_element_type=jnp.float32)
    grad_shared_three = jnp.dot(hidden.T, shared_grad_three, preferred_element_type=jnp.float32)
    shared_dx = jnp.dot(shared_grad_one, shared_one.T, preferred_element_type=jnp.float32) + jnp.dot(shared_grad_three, shared_three.T, preferred_element_type=jnp.float32)

    route_dot = jnp.take_along_axis(dot_acc.reshape(TOKENS_ALL, NUM_EXPERTS), routes, axis=1)
    mean_term = jnp.sum(route_dot * weights, axis=1, keepdims=True) / ROUTE_SCALE
    grad_pick = ROUTE_SCALE / pick_sum * (route_dot - mean_term) * picked * (1.0 - picked)
    grad_logits = jnp.zeros((TOKENS_ALL, NUM_EXPERTS), jnp.float32).at[jnp.arange(TOKENS_ALL)[:, None], routes].set(grad_pick).astype(jnp.bfloat16)
    grad_router = jnp.dot(hidden.T, grad_logits, preferred_element_type=jnp.float32)
    gate_dx = jnp.dot(grad_logits, w_router.T, preferred_element_type=jnp.float32)
    grad_hidden = (grad_f + shared_dx + gate_dx + dx_acc.reshape(TOKENS_ALL, D_MODEL)).astype(jnp.bfloat16)
    return (hidden_out, grad_hidden, grad_router, grad_w_one, grad_w_three, grad_w_two, grad_shared_one, grad_shared_three, grad_shared_two)
```

```python
import functools

import jax
import jax.numpy as jnp
from jax import lax
from jax.experimental import pallas as pl
from jax.experimental.pallas import tpu as pltpu
from jax.sharding import PartitionSpec as P


ROUTE_SCALE = 2.5
STRIDE = 256
VMEM_LIMIT = 60 * 1024 * 1024


def silu_parts(pre_act):
    sig_val = jax.nn.sigmoid(pre_act)
    return pre_act * sig_val, sig_val * (1.0 + pre_act * (1.0 - sig_val))


def route_tables(hidden, routes, w_router, capacity):
    tok_count = hidden.shape[0]
    num_experts = w_router.shape[1]
    logits = jnp.dot(hidden, w_router, preferred_element_type=jnp.float32)
    scores = jax.nn.sigmoid(logits)
    expert_ids = jnp.arange(num_experts, dtype=jnp.int32)
    chosen = routes[:, 0:1] == expert_ids
    for j in range(1, routes.shape[1]):
        chosen = chosen | (routes[:, j : j + 1] == expert_ids)
    picked = jnp.where(chosen, scores, 0.0)
    pick_sum = jnp.sum(picked, axis=1, keepdims=True)
    weights = ROUTE_SCALE * picked / pick_sum
    hit = chosen.astype(jnp.bfloat16)
    rows = lax.broadcasted_iota(jnp.int32, (tok_count, tok_count), 0)
    cols = lax.broadcasted_iota(jnp.int32, (tok_count, tok_count), 1)
    earlier = (cols < rows).astype(jnp.bfloat16)
    before = jnp.dot(earlier, hit, preferred_element_type=jnp.float32)
    kept = chosen & (before < capacity)
    position = jnp.where(kept, before, -1.0)
    return scores, chosen, pick_sum, weights, position


def select_kernel(pos_ref, rows_ref, out_ref, sel_ref):
    tok_count, d_model = rows_ref.shape
    local_experts, capacity, _ = out_ref.shape
    slot_iota = lax.broadcasted_iota(jnp.int32, (capacity, tok_count), 0).astype(jnp.float32)
    for el in range(local_experts):
        hit = slot_iota == pos_ref[0, el : el + 1, :]
        sel_ref[el * capacity : (el + 1) * capacity, :] = jnp.where(hit, 1.0, 0.0).astype(jnp.bfloat16)
    width = 256
    for n in range(d_model // width):
        w = slice(n * width, (n + 1) * width)
        part = jnp.dot(sel_ref[...], rows_ref[:, w], preferred_element_type=jnp.float32).astype(jnp.bfloat16)
        for el in range(local_experts):
            out_ref[el, :, w] = part[el * capacity : (el + 1) * capacity, :]


def select_rows(all_rows, plan, capacity):
    group_size, double, tok_count = plan.shape
    local_experts = double // 2
    d_model = all_rows.shape[1]
    slots = local_experts * capacity
    return pl.pallas_call(
        select_kernel,
        grid=(group_size,),
        in_specs=[
            pl.BlockSpec((1, double, tok_count), lambda g: (g, 0, 0)),
            pl.BlockSpec((tok_count, d_model), lambda g: (g, 0)),
        ],
        out_specs=pl.BlockSpec((local_experts, capacity, d_model), lambda g: (0, g, 0)),
        out_shape=jax.ShapeDtypeStruct((local_experts, group_size * capacity, d_model), jnp.bfloat16),
        scratch_shapes=[pltpu.VMEM((slots, tok_count), jnp.bfloat16)],
        compiler_params=pltpu.CompilerParams(vmem_limit_bytes=VMEM_LIMIT),
        cost_estimate=pl.CostEstimate(flops=2 * group_size * slots * tok_count * d_model, bytes_accessed=2 * group_size * (slots + tok_count) * d_model, transcendentals=0),
    )(plan, all_rows)


def select_grad_kernel(pos_ref, rows_ref, outs_ref, q_ref, dot_ref, sel_ref):
    tok_count, d_model = rows_ref.shape
    local_experts, capacity, _ = q_ref.shape
    slot_iota = lax.broadcasted_iota(jnp.int32, (capacity, tok_count), 0).astype(jnp.float32)
    w_cols = []
    for el in range(local_experts):
        hit = slot_iota == pos_ref[0, el : el + 1, :]
        sel_ref[el * capacity : (el + 1) * capacity, :] = jnp.where(hit, 1.0, 0.0).astype(jnp.bfloat16)
        w_row = pos_ref[0, local_experts + el : local_experts + el + 1, :]
        w_cols.append(jnp.sum(jnp.where(hit, w_row, 0.0), axis=1, keepdims=True))
    dots = [jnp.zeros((capacity, 1), jnp.float32) for _ in range(local_experts)]
    width = 256
    for n in range(d_model // width):
        w = slice(n * width, (n + 1) * width)
        part = jnp.dot(sel_ref[...], rows_ref[:, w], preferred_element_type=jnp.float32)
        for el in range(local_experts):
            grad = part[el * capacity : (el + 1) * capacity, :]
            q_ref[el, :, w] = (w_cols[el] * grad).astype(jnp.bfloat16)
            dots[el] = dots[el] + jnp.sum(grad * outs_ref[0, el, :, w].astype(jnp.float32), axis=1, keepdims=True)
    for el in range(local_experts):
        dot_ref[0, el * capacity : (el + 1) * capacity, :] = jnp.broadcast_to(dots[el], (capacity, 128))


def select_grads(all_grads, plan, expert_outs, capacity):
    group_size, double, tok_count = plan.shape
    local_experts = double // 2
    d_model = all_grads.shape[1]
    slots = local_experts * capacity
    q_rows, slot_dots = pl.pallas_call(
        select_grad_kernel,
        grid=(group_size,),
        in_specs=[
            pl.BlockSpec((1, double, tok_count), lambda g: (g, 0, 0)),
            pl.BlockSpec((tok_count, d_model), lambda g: (g, 0)),
            pl.BlockSpec((1, local_experts, capacity, d_model), lambda g: (g, 0, 0, 0)),
        ],
        out_specs=[pl.BlockSpec((local_experts, capacity, d_model), lambda g: (0, g, 0)), pl.BlockSpec((1, slots, 128), lambda g: (g, 0, 0))],
        out_shape=[jax.ShapeDtypeStruct((local_experts, group_size * capacity, d_model), jnp.bfloat16), jax.ShapeDtypeStruct((group_size, slots, 128), jnp.float32)],
        scratch_shapes=[pltpu.VMEM((slots, tok_count), jnp.bfloat16)],
        compiler_params=pltpu.CompilerParams(vmem_limit_bytes=VMEM_LIMIT),
        cost_estimate=pl.CostEstimate(flops=2 * group_size * slots * tok_count * d_model, bytes_accessed=2 * group_size * (3 * slots + tok_count) * d_model, transcendentals=0),
    )(plan, all_grads, expert_outs)
    return q_rows, slot_dots[:, :, 0]


def forward_kernel(x_ref, one_ref, three_ref, two_ref, pre_one_ref, pre_three_ref, mid_ref, out_ref):
    groups, _, capacity, d_model = out_ref.shape
    pre_one_ref[0] = jnp.dot(x_ref[0], one_ref[0], preferred_element_type=jnp.float32)
    pre_three_ref[0] = jnp.dot(x_ref[0], three_ref[0], preferred_element_type=jnp.float32)

    def middle(r, carry):
        span = pl.ds(pl.multiple_of(r * 48, 48), 48)
        pre_one = pre_one_ref[0, span, :]
        mid_ref[0, span, :] = (pre_one * jax.nn.sigmoid(pre_one) * pre_three_ref[0, span, :]).astype(jnp.bfloat16)
        return carry

    lax.fori_loop(0, groups * capacity // 48, middle, 0)
    width = 256
    for n in range(d_model // width):
        w = slice(n * width, (n + 1) * width)
        part = jnp.dot(mid_ref[0], two_ref[0, :, w], preferred_element_type=jnp.float32).astype(jnp.bfloat16)
        for g in range(groups):
            out_ref[g, 0, :, w] = part[g * capacity : (g + 1) * capacity, :]


def expert_forward(rows, w_one, w_three, w_two, group_size, groups=4):
    local_experts, total, d_model = rows.shape
    d_ff = w_one.shape[2]
    capacity = total // group_size
    tile = groups * capacity
    rows_spec = pl.BlockSpec((1, tile, d_model), lambda e, m: (e, m, 0))
    mid_spec = pl.BlockSpec((1, tile, d_ff), lambda e, m: (e, m, 0))
    up_spec = pl.BlockSpec((1, d_model, d_ff), lambda e, m: (e, 0, 0))
    down_spec = pl.BlockSpec((1, d_ff, d_model), lambda e, m: (e, 0, 0))
    return pl.pallas_call(
        forward_kernel,
        grid=(local_experts, group_size // groups),
        in_specs=[rows_spec, up_spec, up_spec, down_spec],
        out_specs=[mid_spec, mid_spec, mid_spec, pl.BlockSpec((groups, 1, capacity, d_model), lambda e, m: (m, e, 0, 0))],
        out_shape=[
            jax.ShapeDtypeStruct((local_experts, total, d_ff), jnp.float32),
            jax.ShapeDtypeStruct((local_experts, total, d_ff), jnp.float32),
            jax.ShapeDtypeStruct((local_experts, total, d_ff), jnp.bfloat16),
            jax.ShapeDtypeStruct((group_size, local_experts, capacity, d_model), jnp.bfloat16),
        ],
        compiler_params=pltpu.CompilerParams(vmem_limit_bytes=VMEM_LIMIT),
        cost_estimate=pl.CostEstimate(flops=6 * local_experts * total * d_model * d_ff, bytes_accessed=local_experts * total * (4 * d_model + 10 * d_ff), transcendentals=local_experts * total * d_ff),
    )(rows, w_one, w_three, w_two)


def backward_kernel(q_ref, pre_one_ref, pre_three_ref, one_ref, three_ref, two_ref, u_ref, v_ref, dx_ref, mid_ref):
    groups, _, capacity, d_model = dx_ref.shape
    flip = (((1,), (1,)), ((), ()))
    mid_ref[...] = lax.dot_general(q_ref[0], two_ref[0], flip, preferred_element_type=jnp.float32)

    def middle(r, carry):
        span = pl.ds(pl.multiple_of(r * 48, 48), 48)
        pre_one = pre_one_ref[0, span, :]
        grad_mid = mid_ref[span, :]
        act_one, dact_one = silu_parts(pre_one)
        u_ref[0, span, :] = (grad_mid * pre_three_ref[0, span, :] * dact_one).astype(jnp.bfloat16)
        v_ref[0, span, :] = (grad_mid * act_one).astype(jnp.bfloat16)
        return carry

    lax.fori_loop(0, groups * capacity // 48, middle, 0)
    width = 256
    for n in range(d_model // width):
        w = slice(n * width, (n + 1) * width)
        part = lax.dot_general(u_ref[0], one_ref[0, w, :], flip, preferred_element_type=jnp.float32)
        part += lax.dot_general(v_ref[0], three_ref[0, w, :], flip, preferred_element_type=jnp.float32)
        part = part.astype(jnp.bfloat16)
        for g in range(groups):
            dx_ref[g, 0, :, w] = part[g * capacity : (g + 1) * capacity, :]


def expert_backward(q_rows, pre_one, pre_three, w_one, w_three, w_two, group_size, first, count, groups=4):
    _, total, d_model = q_rows.shape
    d_ff = w_one.shape[2]
    capacity = total // group_size
    tile = groups * capacity
    rows_spec = pl.BlockSpec((1, tile, d_model), lambda e, m: (first + e, m, 0))
    mid_spec = pl.BlockSpec((1, tile, d_ff), lambda e, m: (first + e, m, 0))
    new_spec = pl.BlockSpec((1, tile, d_ff), lambda e, m: (e, m, 0))
    up_spec = pl.BlockSpec((1, d_model, d_ff), lambda e, m: (first + e, 0, 0))
    down_spec = pl.BlockSpec((1, d_ff, d_model), lambda e, m: (first + e, 0, 0))
    return pl.pallas_call(
        backward_kernel,
        grid=(count, group_size // groups),
        in_specs=[rows_spec, mid_spec, mid_spec, up_spec, up_spec, down_spec],
        out_specs=[new_spec, new_spec, pl.BlockSpec((groups, 1, capacity, d_model), lambda e, m: (m, e, 0, 0))],
        out_shape=[
            jax.ShapeDtypeStruct((count, total, d_ff), jnp.bfloat16),
            jax.ShapeDtypeStruct((count, total, d_ff), jnp.bfloat16),
            jax.ShapeDtypeStruct((group_size, count, capacity, d_model), jnp.bfloat16),
        ],
        scratch_shapes=[pltpu.VMEM((tile, d_ff), jnp.float32)],
        compiler_params=pltpu.CompilerParams(vmem_limit_bytes=VMEM_LIMIT),
        cost_estimate=pl.CostEstimate(flops=6 * count * total * d_model * d_ff, bytes_accessed=count * total * (4 * d_model + 12 * d_ff), transcendentals=count * total * d_ff),
    )(q_rows, pre_one, pre_three, w_one, w_three, w_two)


def combine_kernel(weighted, first, *refs):
    if weighted:
        cols_ref, dots_ref, rows_ref, acc_ref, tok_dot_ref, stack_ref, t_refs = refs[0], refs[1], refs[2], refs[3], refs[4], refs[5], refs[6:]
    else:
        cols_ref, rows_ref, acc_ref, stack_ref, t_refs = refs[0], refs[1], refs[2], refs[3], refs[4:]
    step = pl.program_id(0)
    segs, capacity, d_model = rows_ref.shape
    tok_count = acc_ref.shape[0]
    tile = t_refs[0].shape[0]

    @pl.when(step == 0)
    def _():
        acc_ref[...] = jnp.zeros_like(acc_ref)
        stack_ref[...] = jnp.zeros_like(stack_ref)
        if weighted:
            tok_dot_ref[...] = jnp.zeros_like(tok_dot_ref)

    for s in range(segs):
        stack_ref[s * STRIDE : s * STRIDE + capacity, :] = rows_ref[s]
    lane_iota = lax.broadcasted_iota(jnp.int32, (tile, STRIDE), 1).astype(jnp.float32)
    if weighted:
        expert_iota = lax.broadcasted_iota(jnp.int32, (tile, tok_dot_ref.shape[1]), 1)

    def body(m, carry):
        span = pl.ds(pl.multiple_of(m * tile, tile), tile)
        cols = cols_ref[0, span, :]
        if weighted:
            dots = jnp.zeros((tile, tok_dot_ref.shape[1]), jnp.float32)
        for s in range(segs):
            hit = lane_iota == cols[:, s : s + 1]
            slots = slice(s * STRIDE, (s + 1) * STRIDE)
            if weighted:
                for k, t_ref in enumerate(t_refs):
                    c = (k + 1) * segs + s
                    t_ref[:, slots] = jnp.where(hit, cols[:, c : c + 1], 0.0).astype(jnp.bfloat16)
                col = jnp.sum(jnp.where(hit, dots_ref[0, s : s + 1, :], 0.0), axis=1, keepdims=True)
                dots = dots + jnp.where(expert_iota == (first + step) * segs + s, col, 0.0)
            else:
                t_refs[0][:, slots] = jnp.where(hit, 1.0, 0.0).astype(jnp.bfloat16)
        if weighted:
            tok_dot_ref[span, :] += dots
        width = 256
        for n in range(d_model // width):
            w = slice(n * width, (n + 1) * width)
            part = jnp.dot(t_refs[0][...], stack_ref[:, w], preferred_element_type=jnp.float32)
            for t_ref in t_refs[1:]:
                part += jnp.dot(t_ref[...], stack_ref[:, w], preferred_element_type=jnp.float32)
            acc_ref[span, w] += part
        return carry

    lax.fori_loop(0, tok_count // tile, body, 0)


def combine(cols, rows, first, steps, dots=None, segs=4, tile=512):
    _, tok_count, width = cols.shape
    _, capacity, d_model = rows.shape
    weighted = dots is not None
    terms = 3 if weighted else 1
    in_specs = [pl.BlockSpec((1, tok_count, width), lambda d: (first + d, 0, 0))]
    args = [cols]
    out_specs = [pl.BlockSpec((tok_count, d_model), lambda d: (0, 0))]
    out_shape = [jax.ShapeDtypeStruct((tok_count, d_model), jnp.float32)]
    if weighted:
        in_specs.append(pl.BlockSpec((1, segs, STRIDE), lambda d: (first + d, 0, 0)))
        args.append(dots)
        out_specs.append(pl.BlockSpec((tok_count, 128), lambda d: (0, 0)))
        out_shape.append(jax.ShapeDtypeStruct((tok_count, 128), jnp.float32))
    in_specs.append(pl.BlockSpec((segs, capacity, d_model), lambda d: (first + d, 0, 0)))
    args.append(rows)
    return pl.pallas_call(
        functools.partial(combine_kernel, weighted, first),
        grid=(steps,),
        in_specs=in_specs,
        out_specs=out_specs,
        out_shape=out_shape,
        scratch_shapes=[pltpu.VMEM((segs * STRIDE, d_model), jnp.bfloat16)] + [pltpu.VMEM((tile, segs * STRIDE), jnp.bfloat16)] * terms,
        compiler_params=pltpu.CompilerParams(vmem_limit_bytes=VMEM_LIMIT),
        cost_estimate=pl.CostEstimate(flops=2 * terms * steps * segs * STRIDE * tok_count * d_model, bytes_accessed=2 * steps * segs * capacity * d_model + 4 * tok_count * d_model, transcendentals=0),
    )(*args)


def shared_forward(hidden, shared_one, shared_three, shared_two):
    pre_one = jnp.dot(hidden, shared_one, preferred_element_type=jnp.float32)
    pre_three = jnp.dot(hidden, shared_three, preferred_element_type=jnp.float32)
    act_one, dact_one = silu_parts(pre_one)
    mid_act = (act_one * pre_three).astype(jnp.bfloat16)
    return jnp.dot(mid_act, shared_two, preferred_element_type=jnp.float32), (pre_three, act_one, dact_one, mid_act)


def shared_backward(hidden, grad_out, saved_acts, shared_one, shared_three, shared_two):
    pre_three, act_one, dact_one, mid_act = saved_acts
    grad_mid = jnp.einsum('td,fd->tf', grad_out, shared_two, preferred_element_type=jnp.float32)
    grad_one = (grad_mid * pre_three * dact_one).astype(jnp.bfloat16)
    grad_three = (grad_mid * act_one).astype(jnp.bfloat16)
    wgrad_one = jnp.einsum('td,tf->df', hidden, grad_one, preferred_element_type=jnp.float32)
    wgrad_three = jnp.einsum('td,tf->df', hidden, grad_three, preferred_element_type=jnp.float32)
    wgrad_two = jnp.einsum('tf,td->fd', mid_act, grad_out, preferred_element_type=jnp.float32)
    dx_part = jnp.einsum('tf,df->td', grad_one, shared_one, preferred_element_type=jnp.float32) + jnp.einsum('tf,df->td', grad_three, shared_three, preferred_element_type=jnp.float32)
    return dx_part, wgrad_one, wgrad_three, wgrad_two


def solution(mesh):
    group_size = mesh.shape['ep']
    row_spec = P('ep', None)
    expert_spec = P('ep', None, None)
    copy_spec = P()

    def layer(hidden, grad_out, routes, w_router, w_one, w_three, w_two, shared_one, shared_three, shared_two):
        tok_count, d_model = hidden.shape
        top_k = routes.shape[1]
        num_experts = w_router.shape[1]
        local_experts = w_one.shape[0]
        capacity = (5 * tok_count * top_k + 4 * num_experts - 1) // (4 * num_experts)
        all_hidden = lax.all_gather(hidden, 'ep', axis=0, tiled=True)
        all_grads = lax.all_gather(grad_out, 'ep', axis=0, tiled=True)

        scores, chosen, pick_sum, weights, position = route_tables(hidden, routes, w_router, capacity)
        pos_t = position.T.reshape(group_size, local_experts, tok_count)
        w_t = weights.T.reshape(group_size, local_experts, tok_count)
        plan = lax.all_to_all(jnp.concatenate([pos_t, w_t], axis=1), 'ep', 0, 0)
        w_hi = lax.reduce_precision(weights, 8, 7)
        w_mid = lax.reduce_precision(weights - w_hi, 8, 7)
        w_low = weights - w_hi - w_mid
        segs = local_experts

        def to_cols(table):
            return table.reshape(tok_count, group_size, segs).transpose(1, 0, 2)

        def part_cols(table, lo, hi):
            part = table.reshape(tok_count, group_size, local_experts)[:, :, lo:hi]
            return part.reshape(tok_count, -1, segs).transpose(1, 0, 2)

        def to_tokens(rows):
            rows = rows.reshape(group_size, -1, d_model)
            return lax.all_to_all(rows, 'ep', 0, 0).reshape(-1, capacity, d_model)

        shared_out, shared_saved = shared_forward(hidden, shared_one, shared_three, shared_two)
        shared_dx, sgrad_one, sgrad_three, sgrad_two = shared_backward(hidden, grad_out, shared_saved, shared_one, shared_three, shared_two)
        grad_shared_one, grad_shared_three, grad_shared_two = lax.psum((sgrad_one, sgrad_three, sgrad_two), 'ep')
        recv_rows = select_rows(all_hidden, plan, capacity)
        pre_one, pre_three, mid_act, expert_out = expert_forward(recv_rows, w_one, w_three, w_two, group_size)
        back_out = to_tokens(expert_out)
        grad_recv, slot_dots = select_grads(all_grads, plan, expert_out, capacity)
        dot_back = lax.all_to_all(slot_dots, 'ep', 0, 0).reshape(group_size, local_experts, capacity)
        dot_back = jnp.pad(dot_back, ((0, 0), (0, 0), (0, STRIDE - capacity)))
        backward = lambda lo, hi: expert_backward(grad_recv, pre_one, pre_three, w_one, w_three, w_two, group_size, lo, hi - lo)
        cut = local_experts - 1
        u_a, v_a, dx_a = backward(0, cut)
        u_b, v_b, dx_b = backward(cut, local_experts)
        dx_back_a = to_tokens(dx_a)
        dx_back_b = to_tokens(dx_b)
        wgrad_two = jnp.einsum('ecf,ecd->efd', mid_act, grad_recv, preferred_element_type=jnp.float32).astype(jnp.bfloat16)

        def wgrad(lo, part):
            return jnp.einsum('ecd,ecf->edf', recv_rows[lo : lo + part.shape[0]], part, preferred_element_type=jnp.float32).astype(jnp.bfloat16)

        wgrad_one = jnp.concatenate([wgrad(0, u_a), wgrad(cut, u_b)])
        wgrad_three = jnp.concatenate([wgrad(0, v_a), wgrad(cut, v_b)])

        cols = jnp.concatenate([to_cols(position), to_cols(w_hi), to_cols(w_mid), to_cols(w_low)], axis=2)
        half = group_size // 2
        routed_a, dots_a = combine(cols, back_out, 0, half, dot_back)
        routed_b, dots_b = combine(cols, back_out, half, half, dot_back)
        routed, dots = routed_a + routed_b, dots_a + dots_b
        hidden_out = (hidden.astype(jnp.float32) + shared_out + routed).astype(jnp.bfloat16)
        route_dot = dots[:, :num_experts]
        mean_term = jnp.sum(route_dot * weights, axis=1, keepdims=True) / ROUTE_SCALE
        grad_pick = ROUTE_SCALE / pick_sum * (route_dot - mean_term) * scores * (1.0 - scores)
        grad_logits = jnp.where(chosen, grad_pick, 0.0).astype(jnp.bfloat16)
        router_part = jnp.einsum('td,te->de', hidden, grad_logits, preferred_element_type=jnp.float32)
        gate_dx = jnp.einsum('te,de->td', grad_logits, w_router, preferred_element_type=jnp.float32)

        dx_routed_a = combine(part_cols(position, 0, cut), dx_back_a, 0, cut * group_size // segs)[0]
        dx_routed_b = combine(part_cols(position, cut, local_experts), dx_back_b, 0, (local_experts - cut) * group_size // segs)[0]
        grad_hidden = (grad_out.astype(jnp.float32) + shared_dx + gate_dx + dx_routed_a + dx_routed_b).astype(jnp.bfloat16)
        grad_router = jnp.sum(lax.all_gather(router_part, 'ep', axis=0), axis=0)
        return (hidden_out, grad_hidden, grad_router, wgrad_one, wgrad_three, wgrad_two, grad_shared_one, grad_shared_three, grad_shared_two)

    return jax.shard_map(layer, mesh=mesh, in_specs=(row_spec, row_spec, row_spec, copy_spec, expert_spec, expert_spec, expert_spec, copy_spec, copy_spec, copy_spec), out_specs=(row_spec, row_spec, copy_spec, expert_spec, expert_spec, expert_spec, copy_spec, copy_spec, copy_spec), check_vma=False)
```
